256 devices in a mesh: rep: 2 (over y_hi), fsdp: 128 (over z, x, y_lo, core).
Axes of the slice: x: 4, y: 4 (y_hi: 2, y_lo: 2; y = y_hi * 2 + y_lo), z: 8, core: 2. Of those that a mesh axis runs over, the one named last changes fastest.
Arguments:
- tokens: bfloat16 [131072, 4096], P(('rep', 'fsdp')), may hold values from -24 to 24
- value_cot: bfloat16 [131072, 1024], P(('rep', 'fsdp')), may hold values from -6 to 6
- value_weight: bfloat16 [2, 4096, 1024], P('rep', 'fsdp'), may hold values from -0.09375 to 0.09375
- global_params: float32 [16777216], P('fsdp'), may hold values from -6 to 6
- local_params: float32 [2, 16777216], P('rep', 'fsdp'), may hold values from -6 to 6
- momentum: float32 [16777216], P('fsdp'), may hold values from -3 to 3
Outputs:
- token_grad: bfloat16 [131072, 4096], P(('rep', 'fsdp'))
- value_grad: float32 [2, 4096, 1024], P('rep', 'fsdp')
- new_global: float32 [16777216], P('fsdp')
- new_moment: float32 [16777216], P('fsdp')
The draws below stay inside these ranges and needn't reach their ends.
All inputs are finite; a program needn't handle non-finite values.
Results may differ from the reference program's by a relative error of at most 0.001.
Values may be sent and summed in bfloat16 or wider, within the bound.
A program may use at most 128 MiB of HBM per device.

```python
import jax
import jax.numpy as jnp
from jax import lax

D = 4096
KVW = 1024
REPS = 2
GROUP_TOK = 65536
TOKENS = 131072
FRAG = 16777216
N_REP = 2


def spiked(drawn, rng, source, target, shards_of, factor):
    def block_of(dim):
        return (jnp.arange(drawn.shape[dim]) // (drawn.shape[dim] // shards_of)).reshape((-1,) + (1,) * (drawn.ndim - 1 - dim))

    first = jax.random.permutation(rng, shards_of)[block_of(target)]
    far = (block_of(target) + shards_of // 2) % shards_of
    return jnp.where((block_of(source) == first) | (block_of(source) == far), factor * drawn, drawn)


def block_levels(stream_key, extent, shards, smallest, top_value):
    def one(dim, shards_of):
        draws = jax.random.uniform(jax.random.fold_in(jax.random.fold_in(stream_key, 6), dim), (shards_of,), jnp.float32, smallest / len(shards), top_value / len(shards))
        return jnp.repeat(jnp.exp(draws), extent[dim] // shards_of).reshape((-1,) + (1,) * (len(extent) - dim - 1))

    level = one(*shards[0])
    for cut in shards[1:]:
        level = level * one(*cut)
    return level


def noise(key, dims, spread, reach, pieces=(), held_as=jnp.bfloat16):
    drawn = spread * jax.random.normal(key, dims, jnp.float32)
    if pieces:
        drawn = drawn * block_levels(key, dims, pieces, -0.22, 0.18)
    return jnp.clip(drawn, -reach, reach).astype(held_as)


def heavy_noise(stream_key, dims, scale, reach, pieces, heavy, dtype=jnp.bfloat16):
    array = scale * jax.random.normal(stream_key, dims, jnp.float32)
    if pieces:
        array = array * block_levels(stream_key, dims, pieces, -0.22, 0.18)
    return jnp.clip(spiked(array, jax.random.fold_in(stream_key, 3), *heavy), -reach, reach).astype(dtype)


def setup_inputs(seed: int = 0) -> dict:
    keys = jax.random.split(jax.random.key(seed), 7)
    return {
        "tokens": heavy_noise(keys[0], (TOKENS, D), 1.0, 24.0, ((0, 256),), (0, 1, 256, 6.0)),
        "value_cot": noise(keys[1], (TOKENS, KVW), 1.0, 6.0, ((0, 256),)),
        "value_weight": noise(keys[2], (REPS, D, KVW), D ** -0.5, 0.09375, ((0, 2), (1, 128))),
        "global_params": noise(keys[3], (FRAG,), 1.0, 6.0, ((0, 128),), jnp.float32),
        "local_params": noise(keys[4], (REPS, FRAG), 1.0, 6.0, ((0, 2), (1, 128)), jnp.float32),
        "momentum": noise(keys[5], (FRAG,), 0.5, 3.0, ((0, 128),), jnp.float32),
    }


def reference(tokens, value_cot, value_weight, global_params, local_params, momentum):
    token_parts = []
    grad_parts = []
    for replica in range(N_REP):
        inputs = tokens[replica * GROUP_TOK:(replica + 1) * GROUP_TOK]
        cotan = value_cot[replica * GROUP_TOK:(replica + 1) * GROUP_TOK]
        token_parts.append(jnp.dot(cotan, value_weight[replica].T, preferred_element_type=jnp.float32).astype(jnp.bfloat16))
        summed = jnp.dot(inputs.T, cotan, preferred_element_type=jnp.float32)
        grad_parts.append(summed * (1.0 / jnp.sqrt(jnp.float32(GROUP_TOK))))
    token_grad = jnp.concatenate(token_parts, axis=0)
    value_grad = jnp.stack(grad_parts, axis=0)
    pseudo = global_params - lax.optimization_barrier(jnp.sum(local_params, axis=0)) / N_REP
    new_moment = 0.9 * momentum + pseudo
    new_global = global_params - 0.7 * (pseudo + 0.9 * new_moment)
    return (token_grad, value_grad, new_global, new_moment)
```

```python
import functools

import jax
import jax.numpy as jnp
from jax import lax
from jax.experimental import pallas as pl
from jax.experimental.pallas import tpu as pltpu
from jax.sharding import Mesh
from jax.sharding import PartitionSpec as P

MESH_ID = pl.DeviceIdType.MESH
AXES = ("rep", "z", "x", "y", "c")
FSDP = AXES[1:]
SIZES = {"z": 8, "x": 4, "y": 2}
ROWS = 32
LANES = 128

RS_ORDERS = ("zxy", "xzy", "yzx", "zxy", "xyz", "yxz", "zyx", "xyz")
AG_CHUNKS = ((0, 2, "xyz"), (2, 1, "zyx"), (3, 1, "zxy"), (4, 2, "zyx"), (6, 1, "xyz"), (7, 1, "zxy"))
PLANES = (4, 5, 3, 6, 2, 7, 1, 0)

SCALE = 2.0 ** -6
LOW = 2.0 ** -8
HIGH = 2.0 ** 8


def encode(v):
    u = v * SCALE
    a = jnp.abs(u)
    p = a * jnp.clip(a, LOW, HIGH)
    p = p * p
    p = p * p
    return jnp.where(u < 0, -p, p).astype(jnp.bfloat16)


def decode(coded):
    y = coded.astype(jnp.float32)
    a = jnp.abs(y)
    r = jnp.sqrt(jnp.sqrt(a))
    m = jnp.sqrt(r)
    v = jnp.where(a < LOW**8, r * (1.0 / LOW), jnp.where(a > HIGH**8, r * (1.0 / HIGH), m))
    v = v * (1.0 / SCALE)
    return jnp.where(y < 0, -v, v)


def arms(n, flip):
    if n == 2:
        return ((1, 1),)
    long, short = n // 2, n - 1 - n // 2
    return ((1, long), (-1, short)) if flip else ((1, short), (-1, long))


def link(dim, sign):
    return dim if SIZES[dim] == 2 else dim + ("+" if sign > 0 else "-")


class Plan:
    RATE = 44e3
    HOP = 2.3

    def __init__(self):
        self.order = []
        self.tc = 0.0
        self.links = {}
        self.ready = []
        self.serial = 0
        self.run()

    def send(self, name, size, rate=None, hop=None):
        begin = max(self.links.get(name, 0.0), self.tc)
        self.links[name] = begin + size / (rate or self.RATE)
        return self.links[name] + (hop or self.HOP)

    def add(self, time, priority, event, duration):
        self.ready.append([time, priority, self.serial, event, duration])
        self.serial += 1

    def rs_nb(self, q, k):
        n = 1
        for d in RS_ORDERS[q][k + 1 :]:
            n *= SIZES[d]
        return n

    def rs_send(self, q, k, sign, j):
        nb = self.rs_nb(q, k)
        d = RS_ORDERS[q][k]
        length = dict(arms(SIZES[d], q % 2))[sign]
        at = self.send(link(d, sign), nb * ROWS * LANES * 2)
        if j + 1 < length:
            self.add(at, 0, ("rs", q, k, sign, j), 0.1 + 0.03 * nb)
        else:
            got = self.last.setdefault((q, k), {})
            got[sign] = at
            if len(got) == len(arms(SIZES[d], q % 2)):
                self.add(max(got.values()), 0, ("fin", q, k), 0.2 + 0.06 * nb)

    def ag_bytes(self, i, k):
        _, tiles, order = AG_CHUNKS[i]
        n = 1
        for d in order[:k]:
            n *= SIZES[d]
        return n * ROWS * LANES * tiles * 2

    def ag_send(self, i, k, sign, j):
        d = AG_CHUNKS[i][2][k]
        at = self.send(link(d, sign), self.ag_bytes(i, k))
        self.add(at, 0, ("ag", i, k, sign, j), 0.03)

    def ag_phase(self, i, k):
        d = AG_CHUNKS[i][2][k]
        for sign, _ in arms(SIZES[d], i % 2):
            self.ag_send(i, k, sign, 0)

    def run(self):
        self.last = {}
        self.tc = 2.0
        self.add(2.0, 0, ("start",), 0.1)
        for n in range(len(PLANES)):
            self.add(3.0, 2 + n, ("mm", n), 0.9)
        seen = {}
        planes = {}
        left = sum(len(AG_CHUNKS) * [sum(s - 1 for s in SIZES.values())])
        while self.ready:
            now = [r for r in self.ready if r[0] <= self.tc]
            if now:
                pick = min(now, key=lambda r: (r[1], r[0], r[2]))
            else:
                pick = min(self.ready, key=lambda r: (r[0], r[1], r[2]))
            self.ready.remove(pick)
            event = pick[3]
            self.tc = max(self.tc, pick[0]) + pick[4]
            self.order.append(event)
            kind = event[0]
            if kind == "start":
                for i in range(len(AG_CHUNKS)):
                    self.ag_phase(i, 0)
                self.add(self.send("y", 524288), 1, ("relay",), 0.05)
            elif kind == "relay":
                self.add(self.send("cross", 524288), 1, ("outer",), 0.6)
            elif kind == "mm":
                planes[PLANES[event[1]]] = self.send("core", 1 << 20, 6e5, 1.0)
                n_all = len(planes) == len(PLANES)
                for q, order in enumerate(RS_ORDERS):
                    for sign, length in arms(SIZES[order[0]], q % 2):
                        if order[0] == "z":
                            if (sign * length) % SIZES["z"] == PLANES[event[1]]:
                                self.add(planes[PLANES[event[1]]], 1, ("go", q, sign), 0.4)
                        elif n_all:
                            self.add(max(planes.values()), 1, ("go", q, sign), 0.1 + 0.03 * self.rs_nb(q, 0))
            elif kind == "go":
                self.rs_send(event[1], 0, event[2], 0)
            elif kind == "rs":
                _, q, k, sign, j = event
                self.rs_send(q, k, sign, j + 1)
            elif kind == "fin":
                _, q, k = event
                if k < 2:
                    for sign, _ in arms(SIZES[RS_ORDERS[q][k + 1]], q % 2):
                        self.rs_send(q, k + 1, sign, 0)
            elif kind == "ag":
                _, i, k, sign, j = event
                d = AG_CHUNKS[i][2][k]
                self.send("core", self.ag_bytes(i, k), 6e5, 1.0)
                if j + 1 < dict(arms(SIZES[d], i % 2))[sign]:
                    self.ag_send(i, k, sign, j + 1)
                seen[i, k] = seen.get((i, k), 0) + 1
                left -= 1
                if seen[i, k] == SIZES[d] - 1 and k < 2:
                    self.ag_phase(i, k + 1)
                if not left:
                    for z in range(SIZES["z"]):
                        self.add(self.tc + 3.0, 3, ("tg", z), 0.9)


def kernel(plan, factor, x_hbm, cot_hbm, w_hbm, g_hbm, l_hbm, m_hbm, tg_hbm, vg_hbm, ng_hbm, nm_hbm,
           xs, cs, w, pb, pp, got, put, tg, vg, g, l, m, mid, other, ng, nm,
           in_sem, out_sem, ag_s, ag_r, fw_s, fw_r, pp_s, pp_r, rs_s, rs_r, rep_s, rep_r):
    at = {name: lax.axis_index(name) for name in AXES}
    me_c = at["c"]

    def peer(**moved):
        return tuple(moved.get(name, at[name]) for name in AXES)

    def towards(dim, sign):
        n = SIZES[dim]
        return peer(**{dim: lax.rem(at[dim] + (sign + n), n)})

    def shifted(dim, by):
        n = SIZES[dim]
        return lax.rem(at[dim] + (by % n), n)

    core = peer(c=1 - me_c)
    across = peer(rep=1 - at["rep"], y=1 - at["y"])
    peers = [core, across]
    for dim in SIZES:
        peers += [towards(dim, sign) for sign, _ in arms(SIZES[dim], 0)]

    local = [
        pltpu.make_async_copy(w_hbm, w.at[at["z"], at["x"], at["y"], me_c], in_sem.at[0]),
        pltpu.make_async_copy(cot_hbm, cs, in_sem.at[1]),
        pltpu.make_async_copy(l_hbm, l, in_sem.at[3]),
        pltpu.make_async_copy(x_hbm, xs, in_sem.at[2]),
        pltpu.make_async_copy(g_hbm, g, in_sem.at[4]),
        pltpu.make_async_copy(m_hbm, m, in_sem.at[5]),
    ]
    for copy in local:
        copy.start()
    barrier = pltpu.get_barrier_semaphore()
    for device in peers:
        pl.semaphore_signal(barrier, inc=1, device_id=device, device_id_type=MESH_ID)
    pl.semaphore_wait(barrier, len(peers))

    def remote(src, dst, send, recv, device):
        return pltpu.make_async_remote_copy(
            src_ref=src, dst_ref=dst, send_sem=send, recv_sem=recv, device_id=device, device_id_type=MESH_ID
        )

    ag_copies, rs_copies, rs_slot = {}, {}, {}
    used = {"ag": 0, "rs": 0, "block": 0}

    def ag_region(i, k, sign, j):
        tile, tiles, order = AG_CHUNKS[i]
        index = {d: slice(None) for d in order[:k]}
        index[order[k]] = shifted(order[k], -sign * j)
        for d in order[k + 1 :]:
            index[d] = at[d]
        return w.at[index["z"], index["x"], index["y"], me_c, :, pl.ds(tile * LANES, tiles * LANES)]

    def ag_send(i, k, sign, j):
        n = used["ag"]
        used["ag"] += 1
        region = ag_region(i, k, sign, j)
        copy = remote(region, region, ag_s.at[n], ag_r.at[n], towards(AG_CHUNKS[i][2][k], sign))
        copy.start()
        ag_copies[i, k, sign, j] = copy

    def ag_phase(i, k):
        for sign, _ in arms(SIZES[AG_CHUNKS[i][2][k]], i % 2):
            ag_send(i, k, sign, 0)

    def nb_of(q, k):
        n = 1
        for d in RS_ORDERS[q][k + 1 :]:
            n *= SIZES[d]
        return n

    def pieces(q, k, dest):
        order = RS_ORDERS[q]
        index = {d: at[d] for d in order[:k]}
        index[order[k]] = dest
        free = sorted(order[k + 1 :], key="zxy".index)
        if not free:
            yield dict(index), 0, 1
        elif len(free) == 1 and SIZES[free[0]] <= 4:
            n = SIZES[free[0]]
            yield {**index, free[0]: slice(None)}, 0, n
        elif len(free) == 1:
            n = SIZES[free[0]]
            for h in range(n // 4):
                yield {**index, free[0]: pl.ds(4 * h, 4)}, 4 * h, 4
        else:
            inner = SIZES[free[1]]
            for o in range(SIZES[free[0]]):
                yield {**index, free[0]: o, free[1]: slice(None)}, o * inner, inner

    def cols(q):
        return pl.ds(q * LANES, LANES)

    def own(q, k, index, n):
        v = pb[index["z"], index["x"], index["y"], me_c, :, cols(q)].reshape(n, ROWS, LANES)
        if k == 0:
            v = v + pp[index["z"], index["x"], index["y"], :, cols(q)].reshape(n, ROWS, LANES)
        return v

    def rs_send(q, k, sign, j):
        d = RS_ORDERS[q][k]
        length = dict(arms(SIZES[d], q % 2))[sign]
        nb = nb_of(q, k)
        base = used["block"]
        used["block"] += nb
        n = used["rs"]
        used["rs"] += 1
        before = rs_slot.get((q, k, sign, j - 1))
        for index, first, count in pieces(q, k, shifted(d, sign * (length - j))):
            v = own(q, k, index, count)
            if before is not None:
                v = v + decode(got[before + first : before + first + count])
            put[base + first : base + first + count] = encode(v)
        copy = remote(put.at[pl.ds(base, nb)], got.at[pl.ds(base, nb)], rs_s.at[n], rs_r.at[n], towards(d, sign))
        copy.start()
        rs_copies[q, k, sign, j] = copy
        rs_slot[q, k, sign, j] = base

    plane_copies = {}
    plane_seen = set()

    def plane_wait(offset):
        if offset not in plane_seen:
            plane_seen.add(offset)
            plane_copies[offset].wait_recv()

    ag_seen = {}
    outs = []
    gathered = [False]
    forwarded = w.at[:, :, :, me_c]
    everything = remote(forwarded, forwarded, fw_s, fw_r, core)
    hop1 = remote(l, mid, rep_s.at[0], rep_r.at[0], towards("y", 1))
    hop2 = remote(mid, other, rep_s.at[1], rep_r.at[1], across)

    for event in plan.order:
        kind = event[0]
        if kind == "start":
            local[0].wait()
            for i in range(len(AG_CHUNKS)):
                ag_phase(i, 0)
            mine = w.at[at["z"], at["x"], at["y"], me_c]
            remote(mine, mine, fw_s, fw_r, core).start()
            local[2].wait()
            hop1.start()
            local[1].wait()
            local[3].wait()
        elif kind == "relay":
            hop1.wait_recv()
            hop2.start()
        elif kind == "outer":
            local[4].wait()
            local[5].wait()
            hop2.wait_recv()
            pseudo = g[...] - (l[...] + other[...]) * 0.5
            moment = 0.9 * m[...] + pseudo
            nm[...] = moment
            ng[...] = g[...] - 0.7 * (pseudo + 0.9 * moment)
            for a, b, s in ((ng, ng_hbm, 0), (nm, nm_hbm, 1)):
                copy = pltpu.make_async_copy(a, b, out_sem.at[s])
                copy.start()
                outs.append(copy)
        elif kind == "mm":
            offset = PLANES[event[1]]
            z = shifted("z", offset)
            width = xs.shape[1] // SIZES["z"]
            rows = xs[:, pl.ds(pl.multiple_of(z * width, width), width)]
            part = lax.dot_general(rows, cs[...], (((0,), (0,)), ((), ())), preferred_element_type=jnp.float32)
            pb[z] = part.reshape(pb.shape[1:])
            copy = remote(pb.at[z, :, :, 1 - me_c], pp.at[z], pp_s.at[event[1]], pp_r.at[event[1]], core)
            copy.start()
            plane_copies[offset] = copy
        elif kind == "go":
            _, q, sign = event
            d = RS_ORDERS[q][0]
            if d == "z":
                plane_wait((sign * dict(arms(SIZES[d], q % 2))[sign]) % SIZES[d])
            else:
                for offset in PLANES:
                    plane_wait(offset)
            rs_send(q, 0, sign, 0)
        elif kind == "rs":
            _, q, k, sign, j = event
            rs_copies[q, k, sign, j].wait_recv()
            d = RS_ORDERS[q][k]
            if k == 0 and d == "z":
                plane_wait((sign * (dict(arms(SIZES[d], q % 2))[sign] - j - 1)) % SIZES[d])
            rs_send(q, k, sign, j + 1)
        elif kind == "fin":
            _, q, k = event
            d = RS_ORDERS[q][k]
            ends = []
            for sign, length in arms(SIZES[d], q % 2):
                rs_copies[q, k, sign, length - 1].wait_recv()
                ends.append(rs_slot[q, k, sign, length - 1])
            if k == 0 and d == "z":
                plane_wait(0)
            for index, first, count in pieces(q, k, at[d]):
                v = own(q, k, index, count)
                for slot in ends:
                    v = v + decode(got[slot + first : slot + first + count])
                if k < 2:
                    spot = pb.at[index["z"], index["x"], index["y"], me_c, :, cols(q)]
                    spot[...] = v.reshape(spot.shape)
                else:
                    vg[:, q * LANES : (q + 1) * LANES] = v.reshape(ROWS, LANES) * factor
            if k < 2:
                for sign, _ in arms(SIZES[RS_ORDERS[q][k + 1]], q % 2):
                    rs_send(q, k + 1, sign, 0)
        elif kind == "ag":
            _, i, k, sign, j = event
            d = AG_CHUNKS[i][2][k]
            ag_copies[i, k, sign, j].wait_recv()
            if j + 1 < dict(arms(SIZES[d], i % 2))[sign]:
                ag_send(i, k, sign, j + 1)
            ag_seen[i, k] = ag_seen.get((i, k), 0) + 1
            if ag_seen[i, k] == SIZES[d] - 1 and k < 2:
                ag_phase(i, k + 1)
            region = ag_region(i, k, sign, j + 1)
            remote(region, region, fw_s, fw_r, core).start()
        elif kind == "tg":
            if not gathered[0]:
                gathered[0] = True
                everything.wait_recv()
            z = event[1]
            width = tg.shape[1] // SIZES["z"]
            part = lax.dot_general(
                cs[...], w[z].reshape(width, w.shape[-1]), (((1,), (1,)), ((), ())), preferred_element_type=jnp.float32
            )
            tg[:, z * width : (z + 1) * width] = part.astype(jnp.bfloat16)
            copy = pltpu.make_async_copy(
                tg.at[:, pl.ds(z * width, width)], tg_hbm.at[:, pl.ds(z * width, width)], out_sem.at[3 + z]
            )
            copy.start()
            outs.append(copy)
    copy = pltpu.make_async_copy(vg, vg_hbm, out_sem.at[2])
    copy.start()
    outs.append(copy)
    for copy in list(ag_copies.values()) + list(rs_copies.values()) + list(plane_copies.values()) + [everything, hop1, hop2]:
        copy.wait_send()
    for copy in outs:
        copy.wait()


def shards(tokens, value_cot, value_weight, global_params, local_params, momentum):
    tok, d = tokens.shape
    kvw = value_cot.shape[1]
    frag = global_params.shape[0]
    flat = (frag // LANES, LANES)
    nz, nx, ny = (SIZES[k] for k in "zxy")
    plan = Plan()
    n_ag = len(AG_CHUNKS) * sum(s - 1 for s in SIZES.values())
    n_rs = len(RS_ORDERS) * sum(s - 1 for s in SIZES.values())
    blocks = len(RS_ORDERS) * (nz * nx * ny - 1)
    f32, bf16 = jnp.float32, jnp.bfloat16
    factor = float((tok * 2 * nz * nx * ny) ** -0.5)
    dma = pltpu.SemaphoreType.DMA
    anywhere = pl.BlockSpec(memory_space=pl.ANY)
    tg, vg, ng, nm = pl.pallas_call(
        functools.partial(kernel, plan, factor),
        out_shape=(
            jax.ShapeDtypeStruct((tok, d), bf16),
            jax.ShapeDtypeStruct((ROWS, kvw), f32),
            jax.ShapeDtypeStruct(flat, f32),
            jax.ShapeDtypeStruct(flat, f32),
        ),
        in_specs=[anywhere] * 6,
        out_specs=(anywhere,) * 4,
        scratch_shapes=[
            pltpu.VMEM((tok, d), bf16),
            pltpu.VMEM((tok, kvw), bf16),
            pltpu.VMEM((nz, nx, ny, 2, ROWS, kvw), bf16),
            pltpu.VMEM((nz, nx, ny, 2, ROWS, kvw), f32),
            pltpu.VMEM((nz, nx, ny, ROWS, kvw), f32),
            pltpu.VMEM((blocks, ROWS, LANES), bf16),
            pltpu.VMEM((blocks, ROWS, LANES), bf16),
            pltpu.VMEM((tok, d), bf16),
            pltpu.VMEM((ROWS, kvw), f32),
        ]
        + [pltpu.VMEM(flat, f32)] * 7
        + [
            dma((6,)),
            dma((3 + nz,)),
            dma((n_ag,)),
            dma((n_ag,)),
            dma,
            dma,
            dma((nz,)),
            dma((nz,)),
            dma((n_rs,)),
            dma((n_rs,)),
            dma((2,)),
            dma((2,)),
        ],
        compiler_params=pltpu.CompilerParams(
            collective_id=0, has_side_effects=True, vmem_limit_bytes=67043328
        ),
        name="step",
    )(
        tokens,
        value_cot,
        value_weight.reshape(ROWS, kvw),
        global_params.reshape(flat),
        local_params.reshape(flat),
        momentum.reshape(flat),
    )
    return tg, vg[None], ng.reshape(frag), nm.reshape(frag)


def solution(mesh):
    n = mesh.shape["fsdp"]
    split = Mesh(mesh.devices.reshape(mesh.shape["rep"], n // 16, 4, 2, 2), AXES)
    return jax.shard_map(
        shards,
        mesh=split,
        in_specs=(
            P(AXES, None),
            P(AXES, None),
            P("rep", FSDP, None),
            P(FSDP),
            P("rep", FSDP),
            P(FSDP),
        ),
        out_specs=(P(AXES, None), P("rep", FSDP, None), P(FSDP), P(FSDP)),
        check_vma=False,
    )
```

```python
import functools

import jax
import jax.numpy as jnp
from jax import lax
from jax.experimental import pallas as pl
from jax.experimental.pallas import tpu as pltpu
from jax.sharding import Mesh
from jax.sharding import PartitionSpec as P

MESH_ID = pl.DeviceIdType.MESH
AXES = ("rep", "z", "x", "y", "c")
FSDP = AXES[1:]
SIZES = {"z": 8, "x": 4, "y": 2}
ROWS = 32
LANES = 128

RS = (("zxy", 0, 0), ("xyz", 1, 0), ("xyz", 0, 0), ("zxy", 1, 1), ("yxz", 0, 1), ("xyz", 1, 1), ("xyz", 0, 1), ("yzx", 0, 1))
AG = ((0, 1, "xzy", 1, 1), (1, 1, "yxz", 1, 3), (2, 1, "yzx", 1, 1), (3, 1, "xyz", 0, 1), (4, 1, "xzy", 1, 0), (5, 1, "yzx", 1, 3), (6, 1, "xyz", 0, 4), (7, 1, "zyx", 0, 4))
PAIRS = (0, 1, 2, 3)

SCALE = 2.0**-3
LOW = 2.0**-4
HIGH = 2.0**10


def encode(v):
    u = v * SCALE
    a = jnp.abs(u)
    p = a * jnp.clip(a, LOW, HIGH)
    p = p * p
    p = p * p
    return jnp.where(u < 0, -p, p).astype(jnp.bfloat16)


def decode(coded):
    y = coded.astype(jnp.float32)
    a = jnp.abs(y)
    r = lax.rsqrt(lax.rsqrt(a))
    m = r * lax.rsqrt(r)
    end = r * jnp.where(a < 1.0, 1.0 / (LOW * SCALE), 1.0 / (HIGH * SCALE))
    v = jnp.where((a < LOW**8) | (a > HIGH**8), end, m * (1.0 / SCALE))
    return jnp.where(y < 0, -v, v)


def arms(n, flip):
    if n == 2:
        return ((1, 1),)
    long, short = n // 2, n - 1 - n // 2
    return ((1, long), (-1, short)) if flip else ((1, short), (-1, long))


def far_first(n):
    return sorted((i if 2 * i <= n else i - n for i in range(1, n)), key=lambda i: (-abs(i), i))


def link(dim, sign):
    return dim if SIZES[dim] == 2 else dim + ("+" if sign > 0 else "-")


class Plan:
    RATE = 44e3
    HOP = 2.4

    def __init__(self, rs=RS, ag=AG, pairs=PAIRS):
        self.rs, self.ag, self.pairs = rs, ag, pairs
        self.order = []
        self.tc = 0.0
        self.links = {}
        self.ready = []
        self.serial = 0
        self.last = {}
        self.held = []
        self.pairs_done = 0
        self.run()

    def send(self, name, size, rate=None, hop=None):
        begin = max(self.links.get(name, 0.0), self.tc)
        self.links[name] = begin + size / (rate or self.RATE)
        return self.links[name] + (hop or self.HOP)

    def add(self, time, priority, event, duration):
        self.ready.append((time, priority, self.serial, event, duration))
        self.serial += 1

    def rs_arms(self, q, k):
        order, flip, straight = self.rs[q]
        n = SIZES[order[k]]
        if k == 2 and straight:
            return tuple((by, 1) for by in far_first(n))
        return arms(n, flip)

    def ag_arms(self, i, k):
        return arms(SIZES[self.ag[i][2][k]], self.ag[i][3])

    def nb(self, q, k):
        n = 1
        for d in self.rs[q][0][k + 1 :]:
            n *= SIZES[d]
        return n

    def rs_send(self, q, k, sign, j):
        nb = self.nb(q, k)
        at = self.send(link(self.rs[q][0][k], sign), abs(sign) * nb * ROWS * LANES * 2)
        at += 0.75 * (abs(sign) - 1)
        if j + 1 < dict(self.rs_arms(q, k))[sign]:
            self.add(at, 0, ("rs", q, k, sign, j), 0.1 + 0.02 * nb)
        else:
            got = self.last.setdefault((q, k), {})
            got[sign] = at
            if len(got) == len(self.rs_arms(q, k)):
                self.add(max(got.values()), 0, ("fin", q, k), 0.15 + 0.05 * nb)

    def ag_bytes(self, i, k):
        n = ROWS * LANES * self.ag[i][1] * 2
        for d in self.ag[i][2][:k]:
            n *= SIZES[d]
        return n

    def ag_send(self, i, k, sign, j):
        at = self.send(link(self.ag[i][2][k], sign), self.ag_bytes(i, k))
        self.add(at, 0, ("ag", i, k, sign, j), 0.05)

    def ag_phase(self, i, k):
        for sign, _ in self.ag_arms(i, k):
            self.ag_send(i, k, sign, 0)

    def release(self):
        for i, k in list(self.held):
            if k < 2 or self.ag[i][4] <= self.pairs_done:
                self.held.remove((i, k))
                self.add(self.tc, 0.5, ("agp", i, k), 0.05)

    def run(self):
        seen = {}
        planes = SIZES["z"]
        pieces = len(self.ag) * sum(n - 1 for n in SIZES.values())
        self.tc = 2.0
        self.add(2.0, 0, ("start",), 0.5)
        for z in range(planes):
            self.add(3.0, 1, ("xt", z), 0.2)
        while self.ready:
            now = [r for r in self.ready if r[0] <= self.tc]
            pick = min(now, key=lambda r: (r[1], r[0], r[2])) if now else min(self.ready)
            self.ready.remove(pick)
            event = pick[3]
            self.tc = max(self.tc, pick[0]) + pick[4]
            self.order.append(event)
            kind = event[0]
            if kind == "start":
                for i in range(len(self.ag)):
                    self.ag_phase(i, 0)
                self.add(self.send("y", 524288), 1, ("relay",), 0.1)
            elif kind == "relay":
                self.add(self.send("cross", 524288), 2, ("outer",), 0.6)
            elif kind == "xt":
                at = self.send("core", 1 << 18, 5e5, 1.0)
                seen["xt"] = seen.get("xt", 0) + 1
                if seen["xt"] == planes:
                    for n, pair in enumerate(self.pairs):
                        self.add(at, 1 + 0.1 * n, ("mm", pair), 0.9)
            elif kind == "mm":
                for q in (2 * event[1], 2 * event[1] + 1):
                    for sign, _ in self.rs_arms(q, 0):
                        self.add(self.tc, 0, ("go", q, sign), 0.1 + 0.02 * self.nb(q, 0))
                self.pairs_done += 1
                self.release()
            elif kind == "agp":
                self.ag_phase(event[1], event[2])
            elif kind == "go":
                self.rs_send(event[1], 0, event[2], 0)
            elif kind == "rs":
                self.rs_send(event[1], event[2], event[3], event[4] + 1)
            elif kind == "fin":
                _, q, k = event
                if k < 2:
                    for sign, _ in self.rs_arms(q, k + 1):
                        self.rs_send(q, k + 1, sign, 0)
            elif kind == "ag":
                _, i, k, sign, j = event
                self.send("core", self.ag_bytes(i, k), 5e5, 1.0)
                if j + 1 < dict(self.ag_arms(i, k))[sign]:
                    self.ag_send(i, k, sign, j + 1)
                seen[i, k] = seen.get((i, k), 0) + 1
                pieces -= 1
                if seen[i, k] == SIZES[self.ag[i][2][k]] - 1 and k < 2:
                    self.held.append((i, k + 1))
                    self.release()
                if not pieces:
                    for z in range(planes):
                        self.add(self.tc + 3.0, 3, ("tg", z), 0.6)


def kernel(plan, factor, x_hbm, cot_hbm, w_hbm, g_hbm, l_hbm, m_hbm, tg, vg, ng, nm,
           xs, cs, xt, px, pc, w, pb, got, put, g, l, m, mid, other,
           in_sem, ag_s, ag_r, fw_s, fw_r, sw_s, sw_r, rs_s, rs_r, rep_s, rep_r):
    at = {name: lax.axis_index(name) for name in AXES}
    me_c = at["c"]

    def peer(**moved):
        return tuple(moved.get(name, at[name]) for name in AXES)

    def towards(dim, sign):
        n = SIZES[dim]
        return peer(**{dim: lax.rem(at[dim] + (sign + n), n)})

    def shifted(dim, by):
        n = SIZES[dim]
        return lax.rem(at[dim] + (by % n), n)

    core = peer(c=1 - me_c)
    across = peer(rep=1 - at["rep"], y=1 - at["y"])
    peers = [core, across]
    for dim in SIZES:
        peers += [towards(dim, sign) for sign, _ in arms(SIZES[dim], 0)]

    local = [
        pltpu.make_async_copy(w_hbm, w.at[at["z"], at["x"], at["y"], me_c], in_sem.at[0]),
        pltpu.make_async_copy(cot_hbm, cs, in_sem.at[1]),
        pltpu.make_async_copy(l_hbm, l, in_sem.at[3]),
        pltpu.make_async_copy(x_hbm, xs, in_sem.at[2]),
        pltpu.make_async_copy(g_hbm, g, in_sem.at[4]),
        pltpu.make_async_copy(m_hbm, m, in_sem.at[5]),
    ]
    for copy in local:
        copy.start()
    barrier = pltpu.get_barrier_semaphore()
    for device in peers:
        pl.semaphore_signal(barrier, inc=1, device_id=device, device_id_type=MESH_ID)
    pl.semaphore_wait(barrier, len(peers))

    def remote(src, dst, send, recv, device):
        return pltpu.make_async_remote_copy(
            src_ref=src, dst_ref=dst, send_sem=send, recv_sem=recv, device_id=device, device_id_type=MESH_ID
        )

    ag_copies, rs_copies, rs_slot = {}, {}, {}
    used = {"ag": 0, "rs": 0, "block": 0}

    def ag_region(i, k, sign, j):
        tile, tiles, order = plan.ag[i][:3]
        index = {d: slice(None) for d in order[:k]}
        index[order[k]] = shifted(order[k], -sign * j)
        for d in order[k + 1 :]:
            index[d] = at[d]
        return w.at[index["z"], index["x"], index["y"], me_c, :, pl.ds(tile * LANES, tiles * LANES)]

    def ag_send(i, k, sign, j):
        n = used["ag"]
        used["ag"] += 1
        region = ag_region(i, k, sign, j)
        copy = remote(region, region, ag_s.at[n], ag_r.at[n], towards(plan.ag[i][2][k], sign))
        copy.start()
        ag_copies[i, k, sign, j] = copy

    def ag_phase(i, k):
        for sign, _ in plan.ag_arms(i, k):
            ag_send(i, k, sign, 0)

    def pieces(q, k, dest):
        order = plan.rs[q][0]
        index = {d: at[d] for d in order[:k]}
        index[order[k]] = dest
        free = sorted(order[k + 1 :], key="zxy".index)
        if not free:
            yield dict(index), 0, 1
        elif len(free) == 1 and SIZES[free[0]] <= 4:
            n = SIZES[free[0]]
            yield {**index, free[0]: slice(None)}, 0, n
        elif len(free) == 1:
            n = SIZES[free[0]]
            for h in range(n // 4):
                yield {**index, free[0]: pl.ds(4 * h, 4)}, 4 * h, 4
        else:
            inner = SIZES[free[1]]
            for o in range(SIZES[free[0]]):
                yield {**index, free[0]: o, free[1]: slice(None)}, o * inner, inner

    def cols(q):
        return pl.ds(q * LANES, LANES)

    def own(q, index, n):
        return pb[index["z"], index["x"], index["y"], :, cols(q)].reshape(n, ROWS, LANES)

    def rs_send(q, k, sign, j):
        d = plan.rs[q][0][k]
        length = dict(plan.rs_arms(q, k))[sign]
        nb = plan.nb(q, k)
        base = used["block"]
        used["block"] += nb
        n = used["rs"]
        used["rs"] += 1
        before = rs_slot.get((q, k, sign, j - 1))
        for index, first, count in pieces(q, k, shifted(d, sign * (length - j))):
            v = own(q, index, count)
            if before is not None:
                v = v + decode(got[before + first : before + first + count])
            put[base + first : base + first + count] = encode(v)
        copy = remote(put.at[pl.ds(base, nb)], got.at[pl.ds(base, nb)], rs_s.at[n], rs_r.at[n], towards(d, sign))
        copy.start()
        rs_copies[q, k, sign, j] = copy
        rs_slot[q, k, sign, j] = base

    swaps = []
    done = set()
    forwarded = w.at[:, :, :, me_c]
    everything = remote(forwarded, forwarded, fw_s, fw_r, core)
    hop1 = remote(l, mid, rep_s.at[0], rep_r.at[0], towards("y", 1))
    hop2 = remote(mid, other, rep_s.at[1], rep_r.at[1], across)
    planes = SIZES["z"]
    width = xs.shape[1] // planes

    for event in plan.order:
        kind = event[0]
        if kind == "start":
            local[0].wait()
            for i in range(len(plan.ag)):
                ag_phase(i, 0)
            mine = w.at[at["z"], at["x"], at["y"], me_c]
            remote(mine, mine, fw_s, fw_r, core).start()
            local[1].wait()
            copy = remote(cs, pc, sw_s.at[planes], sw_r.at[planes], core)
            copy.start()
            swaps.append(copy)
            local[2].wait()
            hop1.start()
            local[3].wait()
        elif kind == "relay":
            hop1.wait_recv()
            hop2.start()
        elif kind == "outer":
            local[4].wait()
            local[5].wait()
            hop2.wait_recv()
            pseudo = g[...] - (l[...] + other[...]) * 0.5
            moment = 0.9 * m[...] + pseudo
            nm[...] = moment
            ng[...] = g[...] - 0.7 * (pseudo + 0.9 * moment)
        elif kind == "xt":
            z = event[1]
            xt[z] = xs[:, z * width : (z + 1) * width].T.reshape(xt.shape[1:])
            copy = remote(xt.at[z, :, :, 1 - me_c], px.at[z], sw_s.at[z], sw_r.at[z], core)
            copy.start()
            swaps.append(copy)
        elif kind == "mm":
            if kind not in done:
                done.add(kind)
                for copy in swaps:
                    copy.wait_recv()
            two = pl.ds(event[1] * 2 * LANES, 2 * LANES)
            half = planes // 2
            for h in (0, half):
                rows = xt[h : h + half, :, :, me_c].reshape(-1, xt.shape[-1])
                more = px[h : h + half].reshape(-1, px.shape[-1])
                part = jnp.dot(rows, cs[:, two], preferred_element_type=jnp.float32)
                part = part + jnp.dot(more, pc[:, two], preferred_element_type=jnp.float32)
                pb[h : h + half, :, :, :, two] = part.reshape((half,) + pb.shape[1:4] + (2 * LANES,))
        elif kind == "agp":
            ag_phase(event[1], event[2])
        elif kind == "go":
            rs_send(event[1], 0, event[2], 0)
        elif kind == "rs":
            _, q, k, sign, j = event
            rs_copies[q, k, sign, j].wait_recv()
            rs_send(q, k, sign, j + 1)
        elif kind == "fin":
            _, q, k = event
            ends = []
            for sign, length in plan.rs_arms(q, k):
                rs_copies[q, k, sign, length - 1].wait_recv()
                ends.append(rs_slot[q, k, sign, length - 1])
            for index, first, count in pieces(q, k, at[plan.rs[q][0][k]]):
                v = own(q, index, count)
                for slot in ends:
                    v = v + decode(got[slot + first : slot + first + count])
                if k < 2:
                    spot = pb.at[index["z"], index["x"], index["y"], :, cols(q)]
                    spot[...] = v.reshape(spot.shape)
                else:
                    vg[:, q * LANES : (q + 1) * LANES] = v.reshape(ROWS, LANES) * factor
            if k < 2:
                for sign, _ in plan.rs_arms(q, k + 1):
                    rs_send(q, k + 1, sign, 0)
        elif kind == "ag":
            _, i, k, sign, j = event
            ag_copies[i, k, sign, j].wait_recv()
            if j + 1 < dict(plan.ag_arms(i, k))[sign]:
                ag_send(i, k, sign, j + 1)
            region = ag_region(i, k, sign, j + 1)
            remote(region, region, fw_s, fw_r, core).start()
        elif kind == "tg":
            if kind not in done:
                done.add(kind)
                everything.wait_recv()
            z = event[1]
            part = lax.dot_general(
                cs[...], w[z].reshape(width, w.shape[-1]), (((1,), (1,)), ((), ())), preferred_element_type=jnp.float32
            )
            tg[:, z * width : (z + 1) * width] = part.astype(jnp.bfloat16)
    for copy in [*ag_copies.values(), *rs_copies.values(), *swaps, everything, hop1, hop2]:
        copy.wait_send()


def finish(*refs):
    n = len(refs) // 2
    sem = refs[-1]
    copies = [pltpu.make_async_copy(refs[i], refs[n + i], sem.at[i]) for i in range(n)]
    for copy in copies:
        copy.start()
    for copy in copies:
        copy.wait()


def shards(tokens, value_cot, value_weight, global_params, local_params, momentum):
    tok, d = tokens.shape
    kvw = value_cot.shape[1]
    frag = global_params.shape[0]
    flat = (frag // LANES, LANES)
    nz, nx, ny = (SIZES[k] for k in "zxy")
    plan = Plan()
    n_ag = len(plan.ag) * sum(s - 1 for s in SIZES.values())
    n_rs = len(plan.rs) * sum(s - 1 for s in SIZES.values())
    blocks = len(plan.rs) * (nz * nx * ny - 1)
    f32, bf16 = jnp.float32, jnp.bfloat16
    factor = float((tok * 2 * nz * nx * ny) ** -0.5)
    dma = pltpu.SemaphoreType.DMA
    anywhere = pl.BlockSpec(memory_space=pl.ANY)
    tg, vg, ng, nm = pl.pallas_call(
        functools.partial(kernel, plan, factor),
        out_shape=(
            pltpu.VMEM((tok, d), bf16),
            pltpu.VMEM((ROWS, kvw), f32),
            pltpu.VMEM(flat, f32),
            pltpu.VMEM(flat, f32),
        ),
        in_specs=[anywhere] * 6,
        out_specs=(pl.BlockSpec(memory_space=pltpu.VMEM),) * 4,
        scratch_shapes=[
            pltpu.VMEM((tok, d), bf16),
            pltpu.VMEM((tok, kvw), bf16),
            pltpu.VMEM((nz, nx, ny, 2, ROWS, tok), bf16),
            pltpu.VMEM((nz, nx, ny, ROWS, tok), bf16),
            pltpu.VMEM((tok, kvw), bf16),
            pltpu.VMEM((nz, nx, ny, 2, ROWS, kvw), bf16),
            pltpu.VMEM((nz, nx, ny, ROWS, kvw), f32),
            pltpu.VMEM((blocks, ROWS, LANES), bf16),
            pltpu.VMEM((blocks, ROWS, LANES), bf16),
        ]
        + [pltpu.VMEM(flat, f32)] * 5
        + [
            dma((6,)),
            dma((n_ag,)),
            dma((n_ag,)),
            dma,
            dma,
            dma((nz + 1,)),
            dma((nz + 1,)),
            dma((n_rs,)),
            dma((n_rs,)),
            dma((2,)),
            dma((2,)),
        ],
        compiler_params=pltpu.CompilerParams(
            collective_id=0, has_side_effects=True, vmem_limit_bytes=58 * 2**20
        ),
        name="step",
    )(
        tokens,
        value_cot,
        value_weight.reshape(ROWS, kvw),
        global_params.reshape(flat),
        local_params.reshape(flat),
        momentum.reshape(flat),
    )
    outs = (tg, vg, ng, nm)
    tg, vg, ng, nm = pl.pallas_call(
        finish,
        out_shape=tuple(jax.ShapeDtypeStruct(o.shape, o.dtype) for o in outs),
        in_specs=[anywhere] * len(outs),
        out_specs=(anywhere,) * len(outs),
        scratch_shapes=[dma((len(outs),))],
        compiler_params=pltpu.CompilerParams(vmem_limit_bytes=2**20),
        name="finish",
    )(*outs)
    return tg, vg[None], ng.reshape(frag), nm.reshape(frag)


def solution(mesh):
    n = mesh.shape["fsdp"]
    split = Mesh(mesh.devices.reshape(mesh.shape["rep"], n // 16, 4, 2, 2), AXES)
    return jax.shard_map(
        shards,
        mesh=split,
        in_specs=(
            P(AXES, None),
            P(AXES, None),
            P("rep", FSDP, None),
            P(FSDP),
            P("rep", FSDP),
            P(FSDP),
        ),
        out_specs=(P(AXES, None), P("rep", FSDP, None), P(FSDP), P(FSDP)),
        check_vma=False,
    )
```

```python
import functools

import jax
import jax.numpy as jnp
from jax import lax
from jax.experimental import pallas as pl
from jax.experimental.pallas import tpu as pltpu
from jax.sharding import Mesh
from jax.sharding import PartitionSpec as P

MESH_ID = pl.DeviceIdType.MESH
AXES = ("rep", "z", "x", "y", "c")
FSDP = AXES[1:]
SIZES = {"z": 8, "x": 4, "y": 2}
ROWS = 32
LANES = 128

RS = (("xyz", 1, 0), ("yzx", 1, 1), ("zyx", 1, 1), ("xzy", 0, 1), ("yzx", 0, 1), ("xzy", 0, 0), ("xzy", 0, 0), ("yzx", 0, 1))
AG = ((0, 1, "yzx", 1, 2), (1, 1, "xzy", 0, 1), (2, 2, "yxz", 1, 1), (4, 1, "xzy", 0, 4), (5, 1, "yzx", 0, 2), (6, 2, "yzx", 1, 0))
PARTS = 2
TILES = 8
PAIRS = (0, 1, 2, 3)
REP = (2.0, 2.0, 2.0, 24.0)

SCALE = 2.0**-3
LOW = 2.0**-4
HIGH = 2.0**10


def encode(v):
    u = v * SCALE
    a = jnp.abs(u)
    p = a * jnp.clip(a, LOW, HIGH)
    p = p * p
    p = p * p
    return jnp.where(u < 0, -p, p).astype(jnp.bfloat16)


def decode(coded):
    y = coded.astype(jnp.float32)
    a = jnp.abs(y)
    r = lax.rsqrt(lax.rsqrt(a))
    m = r * lax.rsqrt(r)
    end = r * jnp.where(a < 1.0, 1.0 / (LOW * SCALE), 1.0 / (HIGH * SCALE))
    v = jnp.where((a < LOW**8) | (a > HIGH**8), end, m * (1.0 / SCALE))
    return jnp.where(y < 0, -v, v)


def arms(n, flip):
    if n == 2:
        return ((1, 1),)
    long, short = n // 2, n - 1 - n // 2
    return ((1, long), (-1, short)) if flip else ((1, short), (-1, long))


def far_first(n):
    return sorted((i if 2 * i <= n else i - n for i in range(1, n)), key=lambda i: (-abs(i), i))


def link(dim, sign):
    return dim if SIZES[dim] == 2 else dim + ("+" if sign > 0 else "-")


class Plan:
    RATE = 44e3
    HOP = 2.4

    def __init__(self, rs=RS, ag=AG, pairs=PAIRS, rep=REP):
        self.rs, self.ag, self.pairs, self.rep = rs, ag, pairs, rep
        self.order = []
        self.tc = 0.0
        self.links = {}
        self.ready = []
        self.serial = 0
        self.last = {}
        self.held = []
        self.pairs_done = 0
        self.parts_done = 0
        self.run()

    def send(self, name, size, rate=None, hop=None):
        begin = max(self.links.get(name, 0.0), self.tc)
        self.links[name] = begin + size / (rate or self.RATE)
        return self.links[name] + (hop or self.HOP)

    def add(self, time, priority, event, duration):
        self.ready.append((time, priority, self.serial, event, duration))
        self.serial += 1

    def part(self, i):
        return self.ag[i][0] * PARTS // TILES

    def rs_arms(self, q, k):
        order, flip, straight = self.rs[q]
        n = SIZES[order[k]]
        if k == 2 and straight:
            return tuple((by, 1) for by in far_first(n))
        return arms(n, flip)

    def ag_arms(self, i, k):
        return arms(SIZES[self.ag[i][2][k]], self.ag[i][3])

    def nb(self, q, k):
        n = 1
        for d in self.rs[q][0][k + 1 :]:
            n *= SIZES[d]
        return n

    def rs_send(self, q, k, sign, j):
        nb = self.nb(q, k)
        at = self.send(link(self.rs[q][0][k], sign), abs(sign) * nb * ROWS * LANES * 2)
        at += 0.75 * (abs(sign) - 1)
        if j + 1 < dict(self.rs_arms(q, k))[sign]:
            self.add(at, 0, ("rs", q, k, sign, j), 0.1 + 0.02 * nb)
        else:
            got = self.last.setdefault((q, k), {})
            got[sign] = at
            if len(got) == len(self.rs_arms(q, k)):
                self.add(max(got.values()), 0, ("fin", q, k), 0.15 + 0.05 * nb)

    def ag_bytes(self, i, k):
        n = ROWS * LANES * self.ag[i][1] * 2
        for d in self.ag[i][2][:k]:
            n *= SIZES[d]
        return n

    def ag_send(self, i, k, sign, j):
        at = self.send(link(self.ag[i][2][k], sign), self.ag_bytes(i, k))
        self.add(at, 0, ("ag", i, k, sign, j), 0.05)

    def ag_phase(self, i, k):
        for sign, _ in self.ag_arms(i, k):
            self.ag_send(i, k, sign, 0)

    def release(self):
        for i, k in list(self.held):
            if k < 2 or self.ag[i][4] <= self.pairs_done:
                self.held.remove((i, k))
                self.add(self.tc, 0.5, ("agp", i, k), 0.05)

    def run(self):
        seen = {}
        planes = SIZES["z"]
        pieces = [0] * PARTS
        for i in range(len(self.ag)):
            pieces[self.part(i)] += sum(n - 1 for n in SIZES.values())
        self.tc = 2.0
        self.add(2.0, 0, ("start",), 0.5)
        for z in range(planes):
            self.add(3.0, 1, ("xt", z), 0.2)
        while self.ready:
            now = [r for r in self.ready if r[0] <= self.tc]
            pick = min(now, key=lambda r: (r[1], r[0], r[2])) if now else min(self.ready)
            self.ready.remove(pick)
            event = pick[3]
            self.tc = max(self.tc, pick[0]) + pick[4]
            self.order.append(event)
            kind = event[0]
            if kind == "start":
                for i in range(len(self.ag)):
                    self.ag_phase(i, 0)
                for n, time in enumerate(self.rep):
                    self.add(max(time, self.tc), 0.2, ("rep", n), 0.05)
            elif kind == "rep":
                self.add(self.send("y", 524288 // len(self.rep)), 1, ("relay", event[1]), 0.05)
            elif kind == "relay":
                self.add(self.send("cross", 524288 // len(self.rep)), 2, ("outer", event[1]), 0.15)
            elif kind == "xt":
                at = self.send("core", 1 << 18, 5e5, 1.0)
                seen["xt"] = seen.get("xt", 0) + 1
                if seen["xt"] == planes:
                    for n, pair in enumerate(self.pairs):
                        self.add(at, 1 + 0.1 * n, ("mm", pair), 0.9)
            elif kind == "mm":
                for q in (2 * event[1], 2 * event[1] + 1):
                    for sign, _ in self.rs_arms(q, 0):
                        self.add(self.tc, 0, ("go", q, sign), 0.1 + 0.02 * self.nb(q, 0))
                self.pairs_done += 1
                self.release()
            elif kind == "agp":
                self.ag_phase(event[1], event[2])
            elif kind == "go":
                self.rs_send(event[1], 0, event[2], 0)
            elif kind == "rs":
                self.rs_send(event[1], event[2], event[3], event[4] + 1)
            elif kind == "fin":
                _, q, k = event
                if k < 2:
                    for sign, _ in self.rs_arms(q, k + 1):
                        self.rs_send(q, k + 1, sign, 0)
            elif kind == "ag":
                _, i, k, sign, j = event
                self.send("core", self.ag_bytes(i, k), 5e5, 1.0)
                if j + 1 < dict(self.ag_arms(i, k))[sign]:
                    self.ag_send(i, k, sign, j + 1)
                seen[i, k] = seen.get((i, k), 0) + 1
                g = self.part(i)
                pieces[g] -= 1
                if seen[i, k] == SIZES[self.ag[i][2][k]] - 1 and k < 2:
                    self.held.append((i, k + 1))
                    self.release()
                if not pieces[g]:
                    self.parts_done += 1
                    for z in range(planes):
                        self.add(self.tc + 2.0, 2 + self.parts_done, ("tg", g, z, self.parts_done), 0.1 + 0.5 / PARTS)


def kernel(plan, factor, x_hbm, cot_hbm, w_hbm, g_hbm, l_hbm, m_hbm, tg, vg, ng, nm,
           xs, cs, xt, px, pc, w, pb, got, put, g, l, m, mid, other, sums,
           in_sem, ag_s, ag_r, fw_s, fw_r, sw_s, sw_r, rs_s, rs_r, rep_s, rep_r):
    at = {name: lax.axis_index(name) for name in AXES}
    me_c = at["c"]

    def peer(**moved):
        return tuple(moved.get(name, at[name]) for name in AXES)

    def towards(dim, sign):
        n = SIZES[dim]
        return peer(**{dim: lax.rem(at[dim] + (sign + n), n)})

    def shifted(dim, by):
        n = SIZES[dim]
        return lax.rem(at[dim] + (by % n), n)

    core = peer(c=1 - me_c)
    across = peer(rep=1 - at["rep"], y=1 - at["y"])
    peers = [core, across]
    for dim in SIZES:
        peers += [towards(dim, sign) for sign, _ in arms(SIZES[dim], 0)]

    local = [
        pltpu.make_async_copy(w_hbm, w.at[at["z"], at["x"], at["y"], me_c], in_sem.at[0]),
        pltpu.make_async_copy(cot_hbm, cs, in_sem.at[1]),
        pltpu.make_async_copy(l_hbm, l, in_sem.at[3]),
        pltpu.make_async_copy(x_hbm, xs, in_sem.at[2]),
        pltpu.make_async_copy(g_hbm, g, in_sem.at[4]),
        pltpu.make_async_copy(m_hbm, m, in_sem.at[5]),
    ]
    for copy in local:
        copy.start()
    barrier = pltpu.get_barrier_semaphore()
    for device in peers:
        pl.semaphore_signal(barrier, inc=1, device_id=device, device_id_type=MESH_ID)
    pl.semaphore_wait(barrier, len(peers))

    def remote(src, dst, send, recv, device):
        return pltpu.make_async_remote_copy(
            src_ref=src, dst_ref=dst, send_sem=send, recv_sem=recv, device_id=device, device_id_type=MESH_ID
        )

    ag_copies, rs_copies, rs_slot = {}, {}, {}
    used = {"ag": 0, "rs": 0, "block": 0}

    def ag_region(i, k, sign, j):
        tile, tiles, order = plan.ag[i][:3]
        index = {d: slice(None) for d in order[:k]}
        index[order[k]] = shifted(order[k], -sign * j)
        for d in order[k + 1 :]:
            index[d] = at[d]
        return w.at[index["z"], index["x"], index["y"], me_c, :, pl.ds(tile * LANES, tiles * LANES)]

    def ag_send(i, k, sign, j):
        n = used["ag"]
        used["ag"] += 1
        region = ag_region(i, k, sign, j)
        copy = remote(region, region, ag_s.at[n], ag_r.at[n], towards(plan.ag[i][2][k], sign))
        copy.start()
        ag_copies[i, k, sign, j] = copy

    def ag_phase(i, k):
        for sign, _ in plan.ag_arms(i, k):
            ag_send(i, k, sign, 0)

    def pieces(q, k, dest):
        order = plan.rs[q][0]
        index = {d: at[d] for d in order[:k]}
        index[order[k]] = dest
        free = sorted(order[k + 1 :], key="zxy".index)
        if not free:
            yield dict(index), 0, 1
        elif len(free) == 1 and SIZES[free[0]] <= 4:
            n = SIZES[free[0]]
            yield {**index, free[0]: slice(None)}, 0, n
        elif len(free) == 1:
            n = SIZES[free[0]]
            for h in range(n // 4):
                yield {**index, free[0]: pl.ds(4 * h, 4)}, 4 * h, 4
        else:
            inner = SIZES[free[1]]
            for o in range(SIZES[free[0]]):
                yield {**index, free[0]: o, free[1]: slice(None)}, o * inner, inner

    def cols(q):
        return pl.ds(q * LANES, LANES)

    def own(q, index, n):
        return pb[index["z"], index["x"], index["y"], :, cols(q)].reshape(n, ROWS, LANES)

    def rs_send(q, k, sign, j):
        d = plan.rs[q][0][k]
        length = dict(plan.rs_arms(q, k))[sign]
        nb = plan.nb(q, k)
        base = used["block"]
        used["block"] += nb
        n = used["rs"]
        used["rs"] += 1
        before = rs_slot.get((q, k, sign, j - 1))
        for index, first, count in pieces(q, k, shifted(d, sign * (length - j))):
            v = own(q, index, count)
            if before is not None:
                v = v + decode(got[before + first : before + first + count])
            put[base + first : base + first + count] = encode(v)
        copy = remote(put.at[pl.ds(base, nb)], got.at[pl.ds(base, nb)], rs_s.at[n], rs_r.at[n], towards(d, sign))
        copy.start()
        rs_copies[q, k, sign, j] = copy
        rs_slot[q, k, sign, j] = base

    swaps = []
    done = set()

    def in_part(n):
        return pl.ds(n * TILES // PARTS * LANES, TILES // PARTS * LANES)

    whole = []
    for n in range(PARTS):
        forwarded = w.at[:, :, :, me_c, :, in_part(n)]
        whole.append(remote(forwarded, forwarded, fw_s.at[n], fw_r.at[n], core))
    n_rep = len(plan.rep)
    share = l.shape[0] // n_rep
    hop1, hop2 = [], []
    for n in range(n_rep):
        rows = pl.ds(n * share, share)
        hop1.append(remote(l.at[rows], mid.at[rows], rep_s.at[n], rep_r.at[n], towards("y", 1)))
        hop2.append(remote(mid.at[rows], other.at[rows], rep_s.at[n_rep + n], rep_r.at[n_rep + n], across))
    planes = SIZES["z"]
    width = xs.shape[1] // planes

    for event in plan.order:
        kind = event[0]
        if kind == "start":
            local[0].wait()
            for i in range(len(plan.ag)):
                ag_phase(i, 0)
            mine = w.at[at["z"], at["x"], at["y"], me_c]
            for n in range(PARTS):
                part = mine.at[:, in_part(n)]
                remote(part, part, fw_s.at[n], fw_r.at[n], core).start()
            local[1].wait()
            copy = remote(cs, pc, sw_s.at[planes], sw_r.at[planes], core)
            copy.start()
            swaps.append(copy)
            local[2].wait()
            local[3].wait()
        elif kind == "rep":
            hop1[event[1]].start()
        elif kind == "relay":
            hop1[event[1]].wait_recv()
            hop2[event[1]].start()
        elif kind == "outer":
            if kind not in done:
                done.add(kind)
                local[4].wait()
                local[5].wait()
            hop2[event[1]].wait_recv()
            rows = pl.ds(event[1] * share, share)
            pseudo = g[rows] - (l[rows] + other[rows]) * 0.5
            moment = 0.9 * m[rows] + pseudo
            nm[rows] = moment
            ng[rows] = g[rows] - 0.7 * (pseudo + 0.9 * moment)
        elif kind == "xt":
            z = event[1]
            xt[z] = xs[:, z * width : (z + 1) * width].T.reshape(xt.shape[1:])
            copy = remote(xt.at[z, :, :, 1 - me_c], px.at[z], sw_s.at[z], sw_r.at[z], core)
            copy.start()
            swaps.append(copy)
        elif kind == "mm":
            if kind not in done:
                done.add(kind)
                for copy in swaps:
                    copy.wait_recv()
            two = pl.ds(event[1] * 2 * LANES, 2 * LANES)
            half = planes // 2
            for h in (0, half):
                rows = xt[h : h + half, :, :, me_c].reshape(-1, xt.shape[-1])
                more = px[h : h + half].reshape(-1, px.shape[-1])
                part = jnp.dot(rows, cs[:, two], preferred_element_type=jnp.float32)
                part = part + jnp.dot(more, pc[:, two], preferred_element_type=jnp.float32)
                pb[h : h + half, :, :, :, two] = part.reshape((half,) + pb.shape[1:4] + (2 * LANES,))
        elif kind == "agp":
            ag_phase(event[1], event[2])
        elif kind == "go":
            rs_send(event[1], 0, event[2], 0)
        elif kind == "rs":
            _, q, k, sign, j = event
            rs_copies[q, k, sign, j].wait_recv()
            rs_send(q, k, sign, j + 1)
        elif kind == "fin":
            _, q, k = event
            ends = []
            for sign, length in plan.rs_arms(q, k):
                rs_copies[q, k, sign, length - 1].wait_recv()
                ends.append(rs_slot[q, k, sign, length - 1])
            for index, first, count in pieces(q, k, at[plan.rs[q][0][k]]):
                v = own(q, index, count)
                for slot in ends:
                    v = v + decode(got[slot + first : slot + first + count])
                if k < 2:
                    spot = pb.at[index["z"], index["x"], index["y"], :, cols(q)]
                    spot[...] = v.reshape(spot.shape)
                else:
                    vg[:, q * LANES : (q + 1) * LANES] = v.reshape(ROWS, LANES) * factor
            if k < 2:
                for sign, _ in plan.rs_arms(q, k + 1):
                    rs_send(q, k + 1, sign, 0)
        elif kind == "ag":
            _, i, k, sign, j = event
            ag_copies[i, k, sign, j].wait_recv()
            if j + 1 < dict(plan.ag_arms(i, k))[sign]:
                ag_send(i, k, sign, j + 1)
            region = ag_region(i, k, sign, j + 1)
            n = plan.part(i)
            remote(region, region, fw_s.at[n], fw_r.at[n], core).start()
        elif kind == "tg":
            _, n, z, turn = event
            if (kind, n) not in done:
                done.add((kind, n))
                whole[n].wait_recv()
            depth = in_part(n)
            part = lax.dot_general(
                cs[:, depth],
                w[z, :, :, :, :, depth].reshape(width, -1),
                (((1,), (1,)), ((), ())),
                preferred_element_type=jnp.float32,
            )
            if turn > 1:
                part = part + sums[z]
            if turn < PARTS:
                sums[z] = part
            else:
                tg[:, z * width : (z + 1) * width] = part.astype(jnp.bfloat16)
    for copy in [*ag_copies.values(), *rs_copies.values(), *swaps, *whole, *hop1, *hop2]:
        copy.wait_send()


def finish(*refs):
    n = len(refs) // 2
    sem = refs[-1]
    copies = [pltpu.make_async_copy(refs[i], refs[n + i], sem.at[i]) for i in range(n)]
    for copy in copies:
        copy.start()
    for copy in copies:
        copy.wait()


def shards(tokens, value_cot, value_weight, global_params, local_params, momentum):
    tok, d = tokens.shape
    kvw = value_cot.shape[1]
    frag = global_params.shape[0]
    flat = (frag // LANES, LANES)
    nz, nx, ny = (SIZES[k] for k in "zxy")
    plan = Plan()
    n_ag = len(plan.ag) * sum(s - 1 for s in SIZES.values())
    n_rs = len(plan.rs) * sum(s - 1 for s in SIZES.values())
    blocks = len(plan.rs) * (nz * nx * ny - 1)
    f32, bf16 = jnp.float32, jnp.bfloat16
    factor = float((tok * 2 * nz * nx * ny) ** -0.5)
    dma = pltpu.SemaphoreType.DMA
    anywhere = pl.BlockSpec(memory_space=pl.ANY)
    tg, vg, ng, nm = pl.pallas_call(
        functools.partial(kernel, plan, factor),
        out_shape=(
            pltpu.VMEM((tok, d), bf16),
            pltpu.VMEM((ROWS, kvw), f32),
            pltpu.VMEM(flat, f32),
            pltpu.VMEM(flat, f32),
        ),
        in_specs=[anywhere] * 6,
        out_specs=(pl.BlockSpec(memory_space=pltpu.VMEM),) * 4,
        scratch_shapes=[
            pltpu.VMEM((tok, d), bf16),
            pltpu.VMEM((tok, kvw), bf16),
            pltpu.VMEM((nz, nx, ny, 2, ROWS, tok), bf16),
            pltpu.VMEM((nz, nx, ny, ROWS, tok), bf16),
            pltpu.VMEM((tok, kvw), bf16),
            pltpu.VMEM((nz, nx, ny, 2, ROWS, kvw), bf16),
            pltpu.VMEM((nz, nx, ny, ROWS, kvw), f32),
            pltpu.VMEM((blocks, ROWS, LANES), bf16),
            pltpu.VMEM((blocks, ROWS, LANES), bf16),
        ]
        + [pltpu.VMEM(flat, f32)] * 5
        + [pltpu.VMEM((nz, tok, d // nz), f32)]
        + [
            dma((6,)),
            dma((n_ag,)),
            dma((n_ag,)),
            dma((PARTS,)),
            dma((PARTS,)),
            dma((nz + 1,)),
            dma((nz + 1,)),
            dma((n_rs,)),
            dma((n_rs,)),
            dma((2 * len(plan.rep),)),
            dma((2 * len(plan.rep),)),
        ],
        compiler_params=pltpu.CompilerParams(
            collective_id=0, has_side_effects=True, vmem_limit_bytes=58 * 2**20
        ),
        name="step",
    )(
        tokens,
        value_cot,
        value_weight.reshape(ROWS, kvw),
        global_params.reshape(flat),
        local_params.reshape(flat),
        momentum.reshape(flat),
    )
    outs = (tg, vg, ng, nm)
    tg, vg, ng, nm = pl.pallas_call(
        finish,
        out_shape=tuple(jax.ShapeDtypeStruct(o.shape, o.dtype) for o in outs),
        in_specs=[anywhere] * len(outs),
        out_specs=(anywhere,) * len(outs),
        scratch_shapes=[dma((len(outs),))],
        compiler_params=pltpu.CompilerParams(vmem_limit_bytes=2**20),
        name="finish",
    )(*outs)
    return tg, vg[None], ng.reshape(frag), nm.reshape(frag)


def solution(mesh):
    n = mesh.shape["fsdp"]
    split = Mesh(mesh.devices.reshape(mesh.shape["rep"], n // 16, 4, 2, 2), AXES)
    return jax.shard_map(
        shards,
        mesh=split,
        in_specs=(
            P(AXES, None),
            P(AXES, None),
            P("rep", FSDP, None),
            P(FSDP),
            P("rep", FSDP),
            P(FSDP),
        ),
        out_specs=(P(AXES, None), P("rep", FSDP, None), P(FSDP), P(FSDP)),
        check_vma=False,
    )
```

```python
import functools

import jax
import jax.numpy as jnp
from jax import lax
from jax.experimental import pallas as pl
from jax.experimental.pallas import tpu as pltpu
from jax.sharding import Mesh
from jax.sharding import PartitionSpec as P

MESH_ID = pl.DeviceIdType.MESH
AXES = ("rep", "z", "x", "y", "c")
FSDP = AXES[1:]
SIZES = {"z": 8, "x": 4, "y": 2}
ROWS = 32
LANES = 128

RS = (("xyz", 1, 0), ("yzx", 1, 1), ("zyx", 1, 1), ("xzy", 0, 1), ("yzx", 0, 1), ("xzy", 0, 0), ("xzy", 0, 0), ("yzx", 0, 1))
AG = ((0, 1, "yzx", 1, 2), (1, 1, "xzy", 0, 1), (2, 2, "yxz", 1, 1), (4, 1, "xzy", 0, 4), (5, 1, "yzx", 0, 2), (6, 2, "yzx", 1, 0))
PARTS = 2
TILES = 8
PAIRS = (0, 1, 2, 3)
REP = (2.0, 2.0, 2.0, 24.0)

SCALE = 2.0**-3
LOW = 2.0**-4
HIGH = 2.0**10


def encode(v):
    u = v * SCALE
    a = jnp.abs(u)
    p = a * jnp.clip(a, LOW, HIGH)
    p = p * p
    p = p * p
    return jnp.where(u < 0, -p, p).astype(jnp.bfloat16)


def decode(coded):
    y = coded.astype(jnp.float32)
    a = jnp.abs(y)
    r = lax.rsqrt(lax.rsqrt(a))
    m = r * lax.rsqrt(r)
    end = r * jnp.where(a < 1.0, 1.0 / (LOW * SCALE), 1.0 / (HIGH * SCALE))
    v = jnp.where((a < LOW**8) | (a > HIGH**8), end, m * (1.0 / SCALE))
    return jnp.where(y < 0, -v, v)


def arms(n, flip):
    if n == 2:
        return ((1, 1),)
    long, short = n // 2, n - 1 - n // 2
    return ((1, long), (-1, short)) if flip else ((1, short), (-1, long))


def far_first(n):
    return sorted((i if 2 * i <= n else i - n for i in range(1, n)), key=lambda i: (-abs(i), i))


def link(dim, sign):
    return dim if SIZES[dim] == 2 else dim + ("+" if sign > 0 else "-")


class Plan:
    RATE = 44e3
    HOP = 2.4

    def __init__(self, rs=RS, ag=AG, pairs=PAIRS, rep=REP):
        self.rs, self.ag, self.pairs, self.rep = rs, ag, pairs, rep
        self.order = []
        self.tc = 0.0
        self.links = {}
        self.ready = []
        self.serial = 0
        self.last = {}
        self.held = []
        self.pairs_done = 0
        self.parts_done = 0
        self.run()

    def send(self, name, size, rate=None, hop=None):
        begin = max(self.links.get(name, 0.0), self.tc)
        self.links[name] = begin + size / (rate or self.RATE)
        return self.links[name] + (hop or self.HOP)

    def add(self, time, priority, event, duration):
        self.ready.append((time, priority, self.serial, event, duration))
        self.serial += 1

    def part(self, i):
        return self.ag[i][0] * PARTS // TILES

    def rs_arms(self, q, k):
        order, flip, straight = self.rs[q]
        n = SIZES[order[k]]
        if k == 2 and straight:
            return tuple((by, 1) for by in far_first(n))
        return arms(n, flip)

    def ag_arms(self, i, k):
        return arms(SIZES[self.ag[i][2][k]], self.ag[i][3])

    def nb(self, q, k):
        n = 1
        for d in self.rs[q][0][k + 1 :]:
            n *= SIZES[d]
        return n

    def rs_send(self, q, k, sign, j):
        nb = self.nb(q, k)
        at = self.send(link(self.rs[q][0][k], sign), abs(sign) * nb * ROWS * LANES * 2)
        at += 0.75 * (abs(sign) - 1)
        if j + 1 < dict(self.rs_arms(q, k))[sign]:
            self.add(at, 0, ("rs", q, k, sign, j), 0.1 + 0.02 * nb)
        else:
            got = self.last.setdefault((q, k), {})
            got[sign] = at
            if len(got) == len(self.rs_arms(q, k)):
                self.add(max(got.values()), 0, ("fin", q, k), 0.15 + 0.05 * nb)

    def ag_bytes(self, i, k):
        n = ROWS * LANES * self.ag[i][1] * 2
        for d in self.ag[i][2][:k]:
            n *= SIZES[d]
        return n

    def ag_send(self, i, k, sign, j):
        at = self.send(link(self.ag[i][2][k], sign), self.ag_bytes(i, k))
        self.add(at, 0, ("ag", i, k, sign, j), 0.05)

    def ag_phase(self, i, k):
        for sign, _ in self.ag_arms(i, k):
            self.ag_send(i, k, sign, 0)

    def release(self):
        for i, k in list(self.held):
            if k < 2 or self.ag[i][4] <= self.pairs_done:
                self.held.remove((i, k))
                self.add(self.tc, 0.5, ("agp", i, k), 0.05)

    def run(self):
        seen = {}
        planes = SIZES["z"]
        pieces = [0] * PARTS
        for i in range(len(self.ag)):
            pieces[self.part(i)] += sum(n - 1 for n in SIZES.values())
        self.tc = 2.0
        self.add(2.0, 0, ("start",), 0.5)
        for z in range(planes):
            self.add(3.0, 1, ("xt", z), 0.2)
        while self.ready:
            now = [r for r in self.ready if r[0] <= self.tc]
            pick = min(now, key=lambda r: (r[1], r[0], r[2])) if now else min(self.ready)
            self.ready.remove(pick)
            event = pick[3]
            self.tc = max(self.tc, pick[0]) + pick[4]
            self.order.append(event)
            kind = event[0]
            if kind == "start":
                for i in range(len(self.ag)):
                    self.ag_phase(i, 0)
                for n, time in enumerate(self.rep):
                    self.add(max(time, self.tc), 0.2, ("rep", n), 0.05)
            elif kind == "rep":
                self.add(self.send("y", 524288 // len(self.rep)), 1, ("relay", event[1]), 0.05)
            elif kind == "relay":
                self.add(self.send("cross", 524288 // len(self.rep)), 2, ("outer", event[1]), 0.15)
            elif kind == "xt":
                at = self.send("core", 1 << 18, 5e5, 1.0)
                seen["xt"] = seen.get("xt", 0) + 1
                if seen["xt"] == planes:
                    for n, pair in enumerate(self.pairs):
                        self.add(at, 1 + 0.1 * n, ("mm", pair), 0.9)
            elif kind == "mm":
                for q in (2 * event[1], 2 * event[1] + 1):
                    for sign, _ in self.rs_arms(q, 0):
                        self.add(self.tc, 0, ("go", q, sign), 0.1 + 0.02 * self.nb(q, 0))
                self.pairs_done += 1
                self.release()
            elif kind == "agp":
                self.ag_phase(event[1], event[2])
            elif kind == "go":
                self.rs_send(event[1], 0, event[2], 0)
            elif kind == "rs":
                self.rs_send(event[1], event[2], event[3], event[4] + 1)
            elif kind == "fin":
                _, q, k = event
                if k < 2:
                    for sign, _ in self.rs_arms(q, k + 1):
                        self.rs_send(q, k + 1, sign, 0)
            elif kind == "ag":
                _, i, k, sign, j = event
                self.send("core", self.ag_bytes(i, k), 5e5, 1.0)
                if j + 1 < dict(self.ag_arms(i, k))[sign]:
                    self.ag_send(i, k, sign, j + 1)
                seen[i, k] = seen.get((i, k), 0) + 1
                g = self.part(i)
                pieces[g] -= 1
                if seen[i, k] == SIZES[self.ag[i][2][k]] - 1 and k < 2:
                    self.held.append((i, k + 1))
                    self.release()
                if not pieces[g]:
                    self.parts_done += 1
                    for z in range(planes):
                        self.add(self.tc + 2.0, 2 + self.parts_done, ("tg", g, z, self.parts_done), 0.1 + 0.5 / PARTS)


def kernel(plan, factor, x_hbm, cot_hbm, w_hbm, g_hbm, l_hbm, m_hbm, tg, vg, ng, nm,
           xs, cs, xt, px, pc, w, pb, got, put, g, l, m, mid, other, sums,
           in_sem, ag_s, ag_r, fw_s, fw_r, sw_s, sw_r, rs_s, rs_r, rep_s, rep_r):
    at = {name: lax.axis_index(name) for name in AXES}
    me_c = at["c"]

    def peer(**moved):
        return tuple(moved.get(name, at[name]) for name in AXES)

    def towards(dim, sign):
        n = SIZES[dim]
        return peer(**{dim: lax.rem(at[dim] + (sign + n), n)})

    def shifted(dim, by):
        n = SIZES[dim]
        return lax.rem(at[dim] + (by % n), n)

    core = peer(c=1 - me_c)
    across = peer(rep=1 - at["rep"], y=1 - at["y"])
    peers = [core, across]
    for dim in SIZES:
        peers += [towards(dim, sign) for sign, _ in arms(SIZES[dim], 0)]

    half_width = xs.shape[1] // 2

    def half_copy(n, sem):
        columns = pl.ds(n * half_width, half_width)
        return pltpu.make_async_copy(x_hbm.at[:, columns], xs.at[:, columns], sem)

    local = [
        pltpu.make_async_copy(w_hbm, w.at[at["z"], at["x"], at["y"], me_c], in_sem.at[0]),
        pltpu.make_async_copy(cot_hbm, cs, in_sem.at[1]),
        half_copy(0, in_sem.at[2]),
        half_copy(1, in_sem.at[6]),
        pltpu.make_async_copy(l_hbm, l, in_sem.at[3]),
        pltpu.make_async_copy(g_hbm, g, in_sem.at[4]),
        pltpu.make_async_copy(m_hbm, m, in_sem.at[5]),
    ]
    for copy in local:
        copy.start()
    barrier = pltpu.get_barrier_semaphore()
    for device in peers:
        pl.semaphore_signal(barrier, inc=1, device_id=device, device_id_type=MESH_ID)
    pl.semaphore_wait(barrier, len(peers))

    def remote(src, dst, send, recv, device):
        return pltpu.make_async_remote_copy(
            src_ref=src, dst_ref=dst, send_sem=send, recv_sem=recv, device_id=device, device_id_type=MESH_ID
        )

    ag_copies, rs_copies, rs_slot = {}, {}, {}
    used = {"ag": 0, "rs": 0, "block": 0}

    def ag_region(i, k, sign, j):
        tile, tiles, order = plan.ag[i][:3]
        index = {d: slice(None) for d in order[:k]}
        index[order[k]] = shifted(order[k], -sign * j)
        for d in order[k + 1 :]:
            index[d] = at[d]
        return w.at[index["z"], index["x"], index["y"], me_c, :, pl.ds(tile * LANES, tiles * LANES)]

    def ag_send(i, k, sign, j):
        n = used["ag"]
        used["ag"] += 1
        region = ag_region(i, k, sign, j)
        copy = remote(region, region, ag_s.at[n], ag_r.at[n], towards(plan.ag[i][2][k], sign))
        copy.start()
        ag_copies[i, k, sign, j] = copy

    def ag_phase(i, k):
        for sign, _ in plan.ag_arms(i, k):
            ag_send(i, k, sign, 0)

    def pieces(q, k, dest):
        order = plan.rs[q][0]
        index = {d: at[d] for d in order[:k]}
        index[order[k]] = dest
        free = sorted(order[k + 1 :], key="zxy".index)
        if not free:
            yield dict(index), 0, 1
        elif len(free) == 1 and SIZES[free[0]] <= 4:
            n = SIZES[free[0]]
            yield {**index, free[0]: slice(None)}, 0, n
        elif len(free) == 1:
            n = SIZES[free[0]]
            for h in range(n // 4):
                yield {**index, free[0]: pl.ds(4 * h, 4)}, 4 * h, 4
        else:
            inner = SIZES[free[1]]
            for o in range(SIZES[free[0]]):
                yield {**index, free[0]: o, free[1]: slice(None)}, o * inner, inner

    def cols(q):
        return pl.ds(q * LANES, LANES)

    def own(q, index, n):
        return pb[index["z"], index["x"], index["y"], :, cols(q)].reshape(n, ROWS, LANES)

    def rs_send(q, k, sign, j):
        d = plan.rs[q][0][k]
        length = dict(plan.rs_arms(q, k))[sign]
        nb = plan.nb(q, k)
        base = used["block"]
        used["block"] += nb
        n = used["rs"]
        used["rs"] += 1
        before = rs_slot.get((q, k, sign, j - 1))
        for index, first, count in pieces(q, k, shifted(d, sign * (length - j))):
            v = own(q, index, count)
            if before is not None:
                v = v + decode(got[before + first : before + first + count])
            put[base + first : base + first + count] = encode(v)
        copy = remote(put.at[pl.ds(base, nb)], got.at[pl.ds(base, nb)], rs_s.at[n], rs_r.at[n], towards(d, sign))
        copy.start()
        rs_copies[q, k, sign, j] = copy
        rs_slot[q, k, sign, j] = base

    swaps = []
    done = set()

    def in_part(n):
        return pl.ds(n * TILES // PARTS * LANES, TILES // PARTS * LANES)

    whole = []
    for n in range(PARTS):
        forwarded = w.at[:, :, :, me_c, :, in_part(n)]
        whole.append(remote(forwarded, forwarded, fw_s.at[n], fw_r.at[n], core))
    n_rep = len(plan.rep)
    share = l.shape[0] // n_rep
    hop1, hop2 = [], []
    for n in range(n_rep):
        rows = pl.ds(n * share, share)
        hop1.append(remote(l.at[rows], mid.at[rows], rep_s.at[n], rep_r.at[n], towards("y", 1)))
        hop2.append(remote(mid.at[rows], other.at[rows], rep_s.at[n_rep + n], rep_r.at[n_rep + n], across))
    planes = SIZES["z"]
    width = xs.shape[1] // planes

    for event in plan.order:
        kind = event[0]
        if kind == "start":
            local[0].wait()
            for i in range(len(plan.ag)):
                ag_phase(i, 0)
            mine = w.at[at["z"], at["x"], at["y"], me_c]
            for n in range(PARTS):
                part = mine.at[:, in_part(n)]
                remote(part, part, fw_s.at[n], fw_r.at[n], core).start()
            local[1].wait()
            copy = remote(cs, pc, sw_s.at[planes], sw_r.at[planes], core)
            copy.start()
            swaps.append(copy)
            local[4].wait()
        elif kind == "rep":
            hop1[event[1]].start()
        elif kind == "relay":
            hop1[event[1]].wait_recv()
            hop2[event[1]].start()
        elif kind == "outer":
            if kind not in done:
                done.add(kind)
                local[5].wait()
                local[6].wait()
            hop2[event[1]].wait_recv()
            rows = pl.ds(event[1] * share, share)
            pseudo = g[rows] - (l[rows] + other[rows]) * 0.5
            moment = 0.9 * m[rows] + pseudo
            nm[rows] = moment
            ng[rows] = g[rows] - 0.7 * (pseudo + 0.9 * moment)
        elif kind == "xt":
            z = event[1]
            if (kind, 2 * z // planes) not in done:
                done.add((kind, 2 * z // planes))
                local[2 + 2 * z // planes].wait()
            xt[z] = xs[:, z * width : (z + 1) * width].T.reshape(xt.shape[1:])
            copy = remote(xt.at[z, :, :, 1 - me_c], px.at[z], sw_s.at[z], sw_r.at[z], core)
            copy.start()
            swaps.append(copy)
        elif kind == "mm":
            if kind not in done:
                done.add(kind)
                for copy in swaps:
                    copy.wait_recv()
            two = pl.ds(event[1] * 2 * LANES, 2 * LANES)
            half = planes // 2
            for h in (0, half):
                rows = xt[h : h + half, :, :, me_c].reshape(-1, xt.shape[-1])
                more = px[h : h + half].reshape(-1, px.shape[-1])
                part = jnp.dot(rows, cs[:, two], preferred_element_type=jnp.float32)
                part = part + jnp.dot(more, pc[:, two], preferred_element_type=jnp.float32)
                pb[h : h + half, :, :, :, two] = part.reshape((half,) + pb.shape[1:4] + (2 * LANES,))
        elif kind == "agp":
            ag_phase(event[1], event[2])
        elif kind == "go":
            rs_send(event[1], 0, event[2], 0)
        elif kind == "rs":
            _, q, k, sign, j = event
            rs_copies[q, k, sign, j].wait_recv()
            rs_send(q, k, sign, j + 1)
        elif kind == "fin":
            _, q, k = event
            ends = []
            for sign, length in plan.rs_arms(q, k):
                rs_copies[q, k, sign, length - 1].wait_recv()
                ends.append(rs_slot[q, k, sign, length - 1])
            for index, first, count in pieces(q, k, at[plan.rs[q][0][k]]):
                v = own(q, index, count)
                for slot in ends:
                    v = v + decode(got[slot + first : slot + first + count])
                if k < 2:
                    spot = pb.at[index["z"], index["x"], index["y"], :, cols(q)]
                    spot[...] = v.reshape(spot.shape)
                else:
                    vg[:, q * LANES : (q + 1) * LANES] = v.reshape(ROWS, LANES) * factor
            if k < 2:
                for sign, _ in plan.rs_arms(q, k + 1):
                    rs_send(q, k + 1, sign, 0)
        elif kind == "ag":
            _, i, k, sign, j = event
            ag_copies[i, k, sign, j].wait_recv()
            if j + 1 < dict(plan.ag_arms(i, k))[sign]:
                ag_send(i, k, sign, j + 1)
            region = ag_region(i, k, sign, j + 1)
            n = plan.part(i)
            remote(region, region, fw_s.at[n], fw_r.at[n], core).start()
        elif kind == "tg":
            _, n, z, turn = event
            if (kind, n) not in done:
                done.add((kind, n))
                whole[n].wait_recv()
            depth = in_part(n)
            part = lax.dot_general(
                cs[:, depth],
                w[z, :, :, :, :, depth].reshape(width, -1),
                (((1,), (1,)), ((), ())),
                preferred_element_type=jnp.float32,
            )
            if turn > 1:
                part = part + sums[z]
            if turn < PARTS:
                sums[z] = part
            else:
                tg[:, z * width : (z + 1) * width] = part.astype(jnp.bfloat16)
    for copy in [*ag_copies.values(), *rs_copies.values(), *swaps, *whole, *hop1, *hop2]:
        copy.wait_send()


def finish(*refs):
    n = len(refs) // 2
    sem = refs[-1]
    copies = [pltpu.make_async_copy(refs[i], refs[n + i], sem.at[i]) for i in range(n)]
    for copy in copies:
        copy.start()
    for copy in copies:
        copy.wait()


def shards(tokens, value_cot, value_weight, global_params, local_params, momentum):
    tok, d = tokens.shape
    kvw = value_cot.shape[1]
    frag = global_params.shape[0]
    flat = (frag // LANES, LANES)
    nz, nx, ny = (SIZES[k] for k in "zxy")
    plan = Plan()
    n_ag = len(plan.ag) * sum(s - 1 for s in SIZES.values())
    n_rs = len(plan.rs) * sum(s - 1 for s in SIZES.values())
    blocks = len(plan.rs) * (nz * nx * ny - 1)
    f32, bf16 = jnp.float32, jnp.bfloat16
    factor = float((tok * 2 * nz * nx * ny) ** -0.5)
    dma = pltpu.SemaphoreType.DMA
    anywhere = pl.BlockSpec(memory_space=pl.ANY)
    tg, vg, ng, nm = pl.pallas_call(
        functools.partial(kernel, plan, factor),
        out_shape=(
            pltpu.VMEM((tok, d), bf16),
            pltpu.VMEM((ROWS, kvw), f32),
            pltpu.VMEM(flat, f32),
            pltpu.VMEM(flat, f32),
        ),
        in_specs=[anywhere] * 6,
        out_specs=(pl.BlockSpec(memory_space=pltpu.VMEM),) * 4,
        scratch_shapes=[
            pltpu.VMEM((tok, d), bf16),
            pltpu.VMEM((tok, kvw), bf16),
            pltpu.VMEM((nz, nx, ny, 2, ROWS, tok), bf16),
            pltpu.VMEM((nz, nx, ny, ROWS, tok), bf16),
            pltpu.VMEM((tok, kvw), bf16),
            pltpu.VMEM((nz, nx, ny, 2, ROWS, kvw), bf16),
            pltpu.VMEM((nz, nx, ny, ROWS, kvw), f32),
            pltpu.VMEM((blocks, ROWS, LANES), bf16),
            pltpu.VMEM((blocks, ROWS, LANES), bf16),
        ]
        + [pltpu.VMEM(flat, f32)] * 5
        + [pltpu.VMEM((nz, tok, d // nz), f32)]
        + [
            dma((7,)),
            dma((n_ag,)),
            dma((n_ag,)),
            dma((PARTS,)),
            dma((PARTS,)),
            dma((nz + 1,)),
            dma((nz + 1,)),
            dma((n_rs,)),
            dma((n_rs,)),
            dma((2 * len(plan.rep),)),
            dma((2 * len(plan.rep),)),
        ],
        compiler_params=pltpu.CompilerParams(
            collective_id=0, has_side_effects=True, vmem_limit_bytes=58 * 2**20
        ),
        name="step",
    )(
        tokens,
        value_cot,
        value_weight.reshape(ROWS, kvw),
        global_params.reshape(flat),
        local_params.reshape(flat),
        momentum.reshape(flat),
    )
    outs = (tg, vg, ng, nm)
    tg, vg, ng, nm = pl.pallas_call(
        finish,
        out_shape=tuple(jax.ShapeDtypeStruct(o.shape, o.dtype) for o in outs),
        in_specs=[anywhere] * len(outs),
        out_specs=(anywhere,) * len(outs),
        scratch_shapes=[dma((len(outs),))],
        compiler_params=pltpu.CompilerParams(vmem_limit_bytes=2**20),
        name="finish",
    )(*outs)
    return tg, vg[None], ng.reshape(frag), nm.reshape(frag)


def solution(mesh):
    n = mesh.shape["fsdp"]
    split = Mesh(mesh.devices.reshape(mesh.shape["rep"], n // 16, 4, 2, 2), AXES)
    return jax.shard_map(
        shards,
        mesh=split,
        in_specs=(
            P(AXES, None),
            P(AXES, None),
            P("rep", FSDP, None),
            P(FSDP),
            P("rep", FSDP),
            P(FSDP),
        ),
        out_specs=(P(AXES, None), P("rep", FSDP, None), P(FSDP), P(FSDP)),
        check_vma=False,
    )
```
